32 devices in a mesh: dom: 16 (over z, x, core), vec: 2 (over y).
Axes of the slice: x: 2, y: 2, z: 4, core: 2. Of those that a mesh axis runs over, the one named last changes fastest.
Arguments:
- orbitals: bfloat16 [128, 65536], P(None, ('dom', 'vec'))
- projectors: bfloat16 [65536, 512], P('dom', 'vec'), may hold values from -0.0234375 to 0.0234375
- potential: float32 [65536], P(('dom', 'vec')), may hold values from 0 to 2
Outputs:
- filtered: bfloat16 [128, 65536], P(None, ('dom', 'vec'))
The draws below stay inside these ranges and needn't reach their ends.
All inputs are finite; a program needn't handle non-finite values.
Results may differ from the reference program's by a relative error of at most 0.0052.
Values may be sent and summed in bfloat16 or wider, within the bound.
No kernel may reach another device: no remote copies, remote signals or barrier semaphores. Data moves between devices by JAX's collectives and lax.ppermute only.
A program may use at most 64 MiB of HBM per device.

```python
import jax
import jax.numpy as jnp
from jax import lax

BANDS = 128
GRID = 65536
VECTORS = 512


def draw_orbitals(key, part):
    key_scale = jax.random.fold_in(key, 11)
    key_values = jax.random.fold_in(key, 12)
    position = jnp.arange(GRID, dtype=jnp.float32) / GRID
    spread = jax.random.uniform(key_scale, (GRID,), jnp.float32)
    amplitude = 3.0 ** (0.5 * position) * 10.0 ** spread
    values = jax.random.normal(key_values, (BANDS, GRID), jnp.float32)
    return (values * amplitude[None, :]).astype(jnp.bfloat16)


def block_scale(rng, extent, split, low, largest):
    def one(axis_at, shards_of):
        heights = jax.random.uniform(jax.random.fold_in(jax.random.fold_in(rng, 6), axis_at), (shards_of,), jnp.float32, low / len(split), largest / len(split))
        return jnp.repeat(jnp.exp(heights), extent[axis_at] // shards_of).reshape((-1,) + (1,) * (len(extent) - axis_at - 1))

    gain = one(*split[0])
    for cut in split[1:]:
        gain = gain * one(*cut)
    return gain


def bell_draw(stream_key, extent, scale, limit, split=(), kind=jnp.bfloat16):
    array = scale * jax.random.normal(stream_key, extent, jnp.float32)
    if split:
        array = array * block_scale(stream_key, extent, split, -0.22, 0.18)
    return jnp.clip(array, -limit, limit).astype(kind)


def setup_inputs(seed: int = 0) -> dict:
    seeds = jax.random.split(jax.random.key(seed), 4)
    return {
        "orbitals": draw_orbitals(jax.random.fold_in(seeds[3], 71), 0),
        "projectors": bell_draw(seeds[1], (GRID, VECTORS), GRID ** -0.5, 0.0234375, ((0, 16), (1, 2))),
        "potential": jnp.clip(2.0 * jax.random.uniform(seeds[2], (GRID,), jnp.float32) ** block_scale(seeds[2], (GRID,), ((0, 32),), -0.2, 0.2), 0.0, 2.0),
    }


CENTER = 1.0
HALF_WIDTH = 1.5
EPSILON = 1e-06

def hamiltonian(bands_now, projectors, shifted):
    intersection = jnp.dot(bands_now, projectors, preferred_element_type=jnp.float32)
    intersection_b = intersection.astype(jnp.bfloat16)
    actions = lax.dot_general(intersection_b, projectors, (((1,), (1,)), ((), ())), preferred_element_type=jnp.float32)
    return (shifted[None, :] * bands_now.astype(jnp.float32) - actions) / HALF_WIDTH

def reference(orbitals, projectors, potential):
    shifted = potential - CENTER
    first_step = hamiltonian(orbitals, projectors, shifted).astype(jnp.bfloat16)
    second = 2.0 * hamiltonian(first_step, projectors, shifted) - orbitals.astype(jnp.float32)
    square_sum = lax.optimization_barrier(jnp.sum(second * second, axis=1))
    scale = lax.rsqrt(square_sum / GRID + EPSILON)
    return (second * scale[:, None]).astype(jnp.bfloat16)
```

```python
import jax
import jax.numpy as jnp
from jax import lax
from jax.sharding import PartitionSpec as P

CENTER = 1.0
HALF_WIDTH = 1.5
EPSILON = 1e-06
F32 = jnp.float32
BF16 = jnp.bfloat16


def shift(value, axis, step):
    size = lax.axis_size(axis)
    return lax.ppermute(value, axis, [(i, (i + step) % size) for i in range(size)])


def sum_over(value, axis):
    size = lax.axis_size(axis)
    if size & (size - 1):
        return lax.psum(value, axis)
    bit = 1
    while bit < size:
        other = lax.ppermute(value.astype(BF16), axis, [(i, i ^ bit) for i in range(size)])
        value = value + other.astype(F32)
        bit *= 2
    return value


def dot(a, b):
    return jnp.dot(a, b, preferred_element_type=F32)


def dot_t(a, b):
    return lax.dot_general(a, b, (((1,), (1,)), ((), ())), preferred_element_type=F32)


def body(orbitals, projectors, potential):
    groups = lax.axis_size("vec")
    mine = lax.axis_index("vec")
    points = orbitals.shape[1]
    axes = ("dom", "vec")
    devices = lax.axis_size(axes)
    shifted = (potential - CENTER)[None, :]

    def rows_of(group):
        return lax.dynamic_slice_in_dim(projectors, group * points, points, 0)

    far_bands = [shift(orbitals, "vec", s) for s in range(1, groups)]
    own = rows_of(mine)
    far_rows = [rows_of((mine + s) % groups) for s in range(1, groups)]
    blocks = [own] + [shift(far_rows[s - 1], "vec", s) for s in range(1, groups)]

    partial = dot(orbitals, own)
    for s in range(1, groups):
        partial = partial + dot(far_bands[s - 1], far_rows[groups - s - 1])
    first_b = sum_over(partial, "dom").astype(BF16)
    firsts = [first_b] + [shift(first_b, "vec", s) for s in range(1, groups)]

    bands = orbitals.astype(F32)
    actions = sum(dot_t(c, b) for c, b in zip(firsts, blocks))
    step = ((shifted * bands - actions) / HALF_WIDTH).astype(BF16)

    partial = dot(step, own)
    for s in range(1, groups):
        partial = partial + shift(dot(step, blocks[s]).astype(BF16), "vec", groups - s).astype(F32)
    second_b = sum_over(partial, "dom").astype(BF16)
    seconds = [second_b] + [shift(second_b, "vec", s) for s in range(1, groups)]

    actions = sum(dot_t(c, b) for c, b in zip(seconds, blocks))
    second = 2.0 * ((shifted * step.astype(F32) - actions) / HALF_WIDTH) - bands
    square = jnp.sum(second * second, axis=1)
    square = lax.all_to_all(jnp.broadcast_to(square, (devices, 1) + square.shape), axes, 0, 0)
    square_sum = jnp.sum(square, axis=(0, 1))
    scale = lax.rsqrt(square_sum / (points * devices) + EPSILON)
    return (second * scale[:, None]).astype(BF16)


def solution(mesh):
    return jax.shard_map(
        body,
        mesh=mesh,
        in_specs=(P(None, ("dom", "vec")), P("dom", "vec"), P(("dom", "vec"))),
        out_specs=P(None, ("dom", "vec")),
        check_vma=False,
    )
```
